128 devices in a mesh: groups: 4 (over y, x), wide: 32 (over z, core).
Axes of the slice: x: 2, y: 2, z: 16, core: 2. Of those that a mesh axis runs over, the one named last changes fastest.
The devices are a block of a 8x8x16 slice.
Arguments:
- alignment_token_ids: int32 [1024, 512], P(('groups', 'wide')), parts along dimension 0, may hold values from 0 to 22
- residue_index_offsets: int32 [2048], P('groups'), parts along dimension 0, may hold values from 0 to 20480, as said below
- target_residue_feature: float32 [2048, 256], P('groups'), parts along dimension 0, may hold values from -6 to 6
- token_embedding_table: float32 [23, 256], replicated, may hold values from -6 to 6
- attention_norm_gain: float32 [256], replicated, may hold values from 0.1 to 1.9
- query_weight: bfloat16 [256, 256], replicated, may hold values from -1 to 1
- key_weight: bfloat16 [256, 256], replicated, may hold values from -25 to 25
- value_weight: bfloat16 [256, 256], replicated, may hold values from -0.375 to 0.375
- gate_weight: bfloat16 [256, 256], replicated, may hold values from -0.375 to 0.375
- gate_offset_bias: float32 [256], replicated, may hold values from -4 to 4
- output_weight: bfloat16 [256, 256], replicated, may hold values from -0.375 to 0.375
- relative_position_table: float32 [65, 8], replicated, may hold values from -4 to 4
- product_norm_gain: float32 [256], replicated, may hold values from 0.1 to 1.9
- left_weight: bfloat16 [256, 32], replicated, may hold values from -0.375 to 0.375
- right_weight: bfloat16 [256, 32], replicated, may hold values from -0.375 to 0.375
- pair_weight: bfloat16 [1024, 128], replicated, may hold values from -0.375 to 0.375
- pair_projection_bias: float32 [128], replicated, may hold values from -3 to 3
Outputs:
- alignment_updated: float32 [1024, 512, 256], P(('groups', 'wide')), parts along dimension 0
- pair: float32 [2048, 512, 128], P(('groups', 'wide')), parts along dimension 0
The draws below stay inside these ranges and needn't reach their ends.
There are 4 independent parts, one for each index of `groups`. The reference program is written for one: setup_inputs(seed, part) draws one part's arguments, and reference() takes and returns one part's arrays. A program takes and returns all parts, laid end to end along the dimension named above; an argument that names none is the same for every part. Nothing has to cross between parts.
Inputs may be any that keep to these rules, and one draw needn't show every extreme that they name: `residue_index_offsets`: rises by 1 from residue to residue within a chain and by more at chain breaks; the first entry is 0 and the last is 20480.
All inputs are finite; a program needn't handle non-finite values.
Results may differ from the reference program's by a relative error of at most 0.0045.
Values may be sent and summed in bfloat16 or wider, within the bound.
A program may use at most 128 MiB of HBM per device.

```python
import math
import jax
import jax.numpy as jnp
import numpy as np
from jax import lax

FEATURE_WIDTH = 256
H = 8
DH = 32
F = 32
P_SIZE = 128
TOKEN_CLASSES = 23
REACH = 32
SEQUENCE_COUNT = 256
RESIDUE_COUNT = 512


def query_key(key):
    first = jnp.clip(jax.random.normal(jax.random.fold_in(key, 101), (FEATURE_WIDTH, H * DH), jnp.float32), -6.0, 6.0) / FEATURE_WIDTH ** 0.5
    second = jnp.clip(jax.random.normal(jax.random.fold_in(key, 202), (FEATURE_WIDTH, H * DH), jnp.float32), -6.0, 6.0) / FEATURE_WIDTH ** 0.5
    return (first, second)


def draw_query_weight(key, part):
    first, second = query_key(key)
    return first.astype(jnp.bfloat16)


def draw_key_weight(key, part):
    first, second = query_key(key)
    result = second
    return result.astype(jnp.bfloat16)


def draw_residue_index_offsets(key, part):
    chance = jax.random.randint(jax.random.fold_in(key, 7), (RESIDUE_COUNT,), 0, 64)
    breaks = jax.random.randint(jax.random.fold_in(key, 8), (RESIDUE_COUNT,), 2, 40)
    stepping = jnp.where(chance == 0, breaks, 1)
    stepping = jnp.where(jnp.arange(RESIDUE_COUNT) == 0, 0, stepping)
    positions = jnp.cumsum(stepping).astype(jnp.int32)
    positions = jnp.where(jnp.arange(RESIDUE_COUNT) == RESIDUE_COUNT - 1, 40 * RESIDUE_COUNT, positions)
    return positions.astype(jnp.int32)


def plant(values, stream_key, least, top_value):
    longest = values.shape.index(max(values.shape))
    spots = []
    for shift in (0, 1):
        where = [jax.random.randint(jax.random.fold_in(stream_key, axis), (), 0, length) for axis, length in enumerate(values.shape)]
        where[longest] = (where[longest] + shift) % values.shape[longest]
        spots.append(tuple(where))
    return values.at[spots[0]].set(least).at[spots[1]].set(top_value)


def rank_table(count, lean):
    portions = [(1 << 20) // math.isqrt(grade ** lean) + 1 for grade in range(1, count + 1)]
    scale = 1 + sum(portions) // (1 << 30)
    return np.cumsum(np.array([max(1, weight // scale) for weight in portions]))


def ranked_ids(key, dims, amount, lean):
    grid = rank_table(amount, lean)
    pick = jax.random.randint(jax.random.fold_in(key, 1), dims, 0, int(grid[amount - 1]))
    rank = jnp.searchsorted(jnp.asarray(grid, jnp.int32), pick, side="right")
    return jax.random.permutation(jax.random.fold_in(key, 2), amount)[rank].astype(jnp.int32)


def gaussian(own_key, shape, scale, most, kind=jnp.bfloat16):
    entries = jax.random.normal(own_key, shape, jnp.float32) * scale
    return jnp.minimum(jnp.maximum(entries, -most), most).astype(kind)


def setup_inputs(seed: int = 0, part: int = 0) -> dict:
    arg_keys = jax.random.split(jax.random.key(seed), 18)
    part_splits = jax.random.split(jax.random.fold_in(arg_keys[17], part), 18)
    return {
        "alignment_token_ids": plant(ranked_ids(part_splits[0], (SEQUENCE_COUNT, RESIDUE_COUNT), TOKEN_CLASSES, 2), jax.random.fold_in(part_splits[0], 3), 0, TOKEN_CLASSES - 1).astype(jnp.int32),
        "residue_index_offsets": draw_residue_index_offsets(jax.random.fold_in(jax.random.fold_in(arg_keys[17], part), 71), part),
        "target_residue_feature": gaussian(part_splits[2], (RESIDUE_COUNT, FEATURE_WIDTH), 1.0, 6.0, jnp.float32),
        "token_embedding_table": gaussian(arg_keys[3], (TOKEN_CLASSES, FEATURE_WIDTH), 1.0, 6.0, jnp.float32),
        "attention_norm_gain": jnp.clip(1.0 + 0.18 * jax.random.normal(arg_keys[4], (FEATURE_WIDTH,), jnp.float32), 0.1, 1.9),
        "query_weight": draw_query_weight(jax.random.fold_in(arg_keys[17], 71), part),
        "key_weight": draw_key_weight(jax.random.fold_in(arg_keys[17], 71), part),
        "value_weight": gaussian(arg_keys[7], (FEATURE_WIDTH, H * DH), FEATURE_WIDTH ** -0.5, 0.375),
        "gate_weight": gaussian(arg_keys[8], (FEATURE_WIDTH, H * DH), FEATURE_WIDTH ** -0.5, 0.375),
        "gate_offset_bias": gaussian(arg_keys[9], (H * DH,), 1.0, 4.0, jnp.float32),
        "output_weight": gaussian(arg_keys[10], (H * DH, FEATURE_WIDTH), (H * DH) ** -0.5, 0.375),
        "relative_position_table": gaussian(arg_keys[11], (2 * REACH + 1, H), 1.0, 4.0, jnp.float32),
        "product_norm_gain": jnp.clip(1.0 + 0.18 * jax.random.normal(arg_keys[12], (FEATURE_WIDTH,), jnp.float32), 0.1, 1.9),
        "left_weight": gaussian(arg_keys[13], (FEATURE_WIDTH, F), FEATURE_WIDTH ** -0.5, 0.375),
        "right_weight": gaussian(arg_keys[14], (FEATURE_WIDTH, F), FEATURE_WIDTH ** -0.5, 0.375),
        "pair_weight": gaussian(arg_keys[15], (F * F, P_SIZE), (F * F // 4) ** -0.5, 0.375),
        "pair_projection_bias": gaussian(arg_keys[16], (P_SIZE,), 0.5, 3.0, jnp.float32),
    }


def layer_normalize(values, gain):
    center = lax.optimization_barrier(jnp.mean(values, axis=-1, keepdims=True))
    centred = values - center
    spread = lax.optimization_barrier(jnp.mean(centred * centred, axis=-1, keepdims=True))
    return centred * lax.rsqrt(spread + 1e-05) * gain

def reference(alignment_token_ids, residue_index_offsets, target_residue_feature, token_embedding_table, attention_norm_gain, query_weight, key_weight, value_weight, gate_weight, gate_offset_bias, output_weight, relative_position_table, product_norm_gain, left_weight, right_weight, pair_weight, pair_projection_bias):
    alignment_initial = token_embedding_table[alignment_token_ids] + target_residue_feature[None, :, :]
    offsets = jnp.clip(residue_index_offsets[None, :] - residue_index_offsets[:, None], -REACH, REACH) + REACH
    offset_bias = jnp.transpose(relative_position_table[offsets], (2, 0, 1))

    def row_attention_step(row):
        normed = layer_normalize(row, attention_norm_gain).astype(jnp.bfloat16)
        query = (jnp.dot(normed, query_weight, preferred_element_type=jnp.float32) / DH ** 0.5).astype(jnp.bfloat16)
        keys = jnp.dot(normed, key_weight, preferred_element_type=jnp.float32).astype(jnp.bfloat16)
        values = jnp.dot(normed, value_weight, preferred_element_type=jnp.float32).astype(jnp.bfloat16)
        gate = jax.nn.sigmoid(jnp.dot(normed, gate_weight, preferred_element_type=jnp.float32) + gate_offset_bias)
        query_heads = query.reshape(RESIDUE_COUNT, H, DH).astype(jnp.float32)
        key_heads = keys.reshape(RESIDUE_COUNT, H, DH).astype(jnp.float32)
        value_heads = values.reshape(RESIDUE_COUNT, H, DH).astype(jnp.float32)
        scores = jnp.einsum('ihd,jhd->hij', query_heads, key_heads, precision=lax.Precision.HIGHEST) + offset_bias
        scores = scores - lax.optimization_barrier(jnp.max(scores, axis=-1, keepdims=True))
        expo = jnp.exp(scores)
        weights = (expo / lax.optimization_barrier(jnp.sum(expo, axis=-1, keepdims=True))).astype(jnp.bfloat16)
        mixed = jnp.einsum('hij,jhd->ihd', weights.astype(jnp.float32), value_heads, precision=lax.Precision.HIGHEST)
        mixed = (mixed.reshape(RESIDUE_COUNT, H * DH) * gate).astype(jnp.bfloat16)
        return row + jnp.dot(mixed, output_weight, preferred_element_type=jnp.float32)
    alignment_updated = lax.map(row_attention_step, alignment_initial)
    normalized_second = layer_normalize(alignment_updated, product_norm_gain).astype(jnp.bfloat16).reshape(SEQUENCE_COUNT * RESIDUE_COUNT, FEATURE_WIDTH)
    left = jnp.dot(normalized_second, left_weight, preferred_element_type=jnp.float32).astype(jnp.bfloat16).reshape(SEQUENCE_COUNT, RESIDUE_COUNT, F)
    right = jnp.dot(normalized_second, right_weight, preferred_element_type=jnp.float32).astype(jnp.bfloat16).reshape(SEQUENCE_COUNT, RESIDUE_COUNT, F)
    right_wide = right.astype(jnp.float32)
    blocks = jnp.transpose(left.reshape(SEQUENCE_COUNT, RESIDUE_COUNT // 16, 16, F), (1, 0, 2, 3))

    def rows(block):
        outer = jnp.einsum('sic,sje->ijce', block.astype(jnp.float32), right_wide, precision=lax.Precision.HIGHEST) / SEQUENCE_COUNT
        flat = outer.reshape(16 * RESIDUE_COUNT, F * F).astype(jnp.bfloat16)
        return (jnp.dot(flat, pair_weight, preferred_element_type=jnp.float32) + pair_projection_bias).reshape(16, RESIDUE_COUNT, P_SIZE)
    pair = lax.map(rows, blocks).reshape(RESIDUE_COUNT, RESIDUE_COUNT, P_SIZE)
    return (alignment_updated, pair)
```

```python
import functools

import jax
import jax.numpy as jnp
from jax import lax
from jax.experimental import pallas as pl
from jax.experimental.pallas import tpu as pltpu
from jax.sharding import PartitionSpec as P

REACH = 32
LANES = 128
F32 = jnp.float32
BF16 = jnp.bfloat16


def dot(a, b):
    return lax.dot_general(a, b, (((1,), (0,)), ((), ())), preferred_element_type=F32)


def dot_tb(a, b):
    return lax.dot_general(a, b, (((1,), (1,)), ((), ())), preferred_element_type=F32)


def dot_ta(a, b):
    return lax.dot_general(a, b, (((0,), (0,)), ((), ())), preferred_element_type=F32)


def layer_normalize(values, gain):
    center = jnp.mean(values, axis=-1, keepdims=True)
    centred = values - center
    spread = jnp.mean(centred * centred, axis=-1, keepdims=True)
    return centred * lax.rsqrt(spread + 1e-05) * gain


def attention_kernel(
    heads,
    tok_ref,
    pos_row_ref,
    pos_col_ref,
    target_ref,
    emb_ref,
    gain_one_ref,
    wq_ref,
    wk_ref,
    wv_ref,
    wg_ref,
    gb_ref,
    wo_ref,
    table_ref,
    gain_two_ref,
    wl_ref,
    wr_ref,
    au_ref,
    left_ref,
    right_ref,
    bias_ref,
    emb3_ref,
    score_ref,
    prob_ref,
    mixed_ref,
    left_acc,
    right_acc,
):
    seq = pl.program_id(0)
    residues, features = target_ref.shape
    classes = emb_ref.shape[0]
    head_size = features // heads
    per_half = LANES // head_size

    @pl.when(seq == 0)
    def _():
        @pl.loop(0, residues // 8)
        def _(block):
            rows = pl.ds(pl.multiple_of(block * 8, 8), 8)
            delta = pos_row_ref[...] - pos_col_ref[rows, :]
            offs = jnp.clip(delta, -REACH, REACH) + REACH
            for h in range(heads):
                source = jnp.broadcast_to(table_ref[h : h + 1, :], (8, LANES))
                for col in range(residues // LANES):
                    cols = slice(col * LANES, (col + 1) * LANES)
                    bias_ref[h, rows, cols] = jnp.take_along_axis(
                        source, offs[:, cols], axis=1, mode="promise_in_bounds"
                    )

        emb3_ref[...] = jnp.zeros_like(emb3_ref)
        rest = emb_ref[...]
        for part in range(3):
            piece = rest.astype(BF16)
            emb3_ref[part * 32 : part * 32 + classes, :] = piece
            rest = rest - piece.astype(F32)
        left_acc[...] = jnp.zeros_like(left_acc)

    token = tok_ref[pl.ds(seq, 1), :]
    klass = lax.broadcasted_iota(jnp.int32, (LANES, residues), 0)
    onehot = jnp.where((klass % 32 == token) & (klass < 96), 1.0, 0.0).astype(BF16)
    start = dot_ta(onehot, emb3_ref[...]) + target_ref[...]
    normed = layer_normalize(start, gain_one_ref[...]).astype(BF16)
    query = (dot(normed, wq_ref[...]) * (1.0 / head_size**0.5)).astype(BF16)
    keys = dot(normed, wk_ref[...]).astype(BF16)
    values = dot(normed, wv_ref[...]).astype(BF16)
    lane = lax.broadcasted_iota(jnp.int32, (residues, features), 1) // head_size
    half_lane = lax.broadcasted_iota(jnp.int32, (residues, LANES), 1) // head_size
    ones = jnp.ones((residues, LANES), BF16)
    for h in range(heads):
        half, place = divmod(h, per_half)
        masked = jnp.where(lane == h, query, jnp.zeros_like(query))
        score_ref[h % 2] = dot_tb(masked, keys)
        for block in range(residues // LANES):
            rows = slice(block * LANES, (block + 1) * LANES)
            scores = score_ref[h % 2, rows, :] + bias_ref[h, rows, :]
            peak = jnp.max(scores, axis=1, keepdims=True)
            prob_ref[h % 2, rows, :] = jnp.exp(scores - peak).astype(BF16)
        extended = jnp.concatenate([values[:, half * LANES : (half + 1) * LANES], ones], axis=1)
        product = dot(prob_ref[h % 2], extended)
        result = product[:, :LANES] / product[:, LANES:]
        cols = slice(half * LANES, (half + 1) * LANES)
        if place == 0:
            mixed_ref[:, cols] = result
        else:
            mixed_ref[:, cols] = jnp.where(half_lane == place, result, mixed_ref[:, cols])
    gate = jax.nn.sigmoid(dot(normed, wg_ref[...]) + gb_ref[...])
    mixed = (mixed_ref[...] * gate).astype(BF16)
    updated = start + dot(mixed, wo_ref[...])
    au_ref[0] = updated
    second = layer_normalize(updated, gain_two_ref[...]).astype(BF16)
    group = seq // 4
    rows = pl.ds(pl.multiple_of(group * residues, residues), residues)
    left_acc[rows, :] += dot(second, wl_ref[seq % 4])
    right = dot_tb(wr_ref[...], second)
    for col in range(residues // LANES):
        right_acc[col, pl.ds(seq, 32, stride=8), :] = right[:, col * LANES : (col + 1) * LANES]

    @pl.when(seq == pl.num_programs(0) - 1)
    def _():
        devices, groups, owned, _ = left_ref.shape
        for g in range(groups):
            part = left_acc[g * residues : (g + 1) * residues, :].astype(BF16)
            left_ref[:, g] = part.reshape(devices, owned, LANES)
        for col in range(residues // LANES):
            right_ref[:, col * LANES : (col + 1) * LANES] = right_acc[col].astype(BF16)


def attention(
    devices,
    tokens,
    positions,
    target,
    emb,
    gain_one,
    wq,
    wk,
    wv,
    wg,
    gb,
    wo,
    table,
    gain_two,
    wl,
    wr,
):
    sequences, residues = tokens.shape
    features = target.shape[1]
    heads = table.shape[1]
    width = wl.shape[1]
    table_rows = jnp.pad(table.T, ((0, 0), (0, LANES - table.shape[0])))
    wl4 = jnp.stack([jnp.pad(wl, ((0, 0), (k * width, LANES - (k + 1) * width))) for k in range(4)])
    operands = (
        tokens,
        positions[None, :],
        positions[:, None],
        target,
        emb,
        gain_one[None, :],
        wq,
        wk,
        wv,
        wg,
        gb[None, :],
        wo,
        table_rows,
        gain_two[None, :],
        wl4,
        wr.T,
    )
    owned = residues // devices

    def const(a):
        return pl.BlockSpec(a.shape, lambda s: (0,) * a.ndim)

    return pl.pallas_call(
        functools.partial(attention_kernel, heads),
        grid=(sequences,),
        in_specs=[const(a) for a in operands],
        out_specs=(
            pl.BlockSpec((1, residues, features), lambda s: (s, 0, 0)),
            pl.BlockSpec((devices, 2, owned, LANES), lambda s: (0, 0, 0, 0)),
            pl.BlockSpec((width * sequences, residues), lambda s: (0, 0)),
        ),
        out_shape=(
            jax.ShapeDtypeStruct((sequences, residues, features), F32),
            jax.ShapeDtypeStruct((devices, 2, owned, LANES), BF16),
            jax.ShapeDtypeStruct((width * sequences, residues), BF16),
        ),
        scratch_shapes=[
            pltpu.VMEM((heads, residues, residues), F32),
            pltpu.VMEM((LANES, features), BF16),
            pltpu.VMEM((2, residues, residues), F32),
            pltpu.VMEM((2, residues, residues), BF16),
            pltpu.VMEM((residues, features), F32),
            pltpu.VMEM((2 * residues, LANES), F32),
            pltpu.VMEM((residues // LANES, width * sequences, LANES), F32),
        ],
        compiler_params=pltpu.CompilerParams(
            dimension_semantics=("arbitrary",), vmem_limit_bytes=60 << 20
        ),
        cost_estimate=pl.CostEstimate(
            flops=20_000_000_000, bytes_accessed=8 << 20, transcendentals=17_000_000
        ),
        name="row_attention",
    )(*operands)


def exchange_kernel(
    devices,
    chunks,
    lag,
    left_ref,
    right_ref,
    weight_ref,
    bias_ref,
    pair_ref,
    held_ref,
    left_held,
    left_wide,
    left_rows,
    y_ref,
    acc_ref,
    send_sem,
    up_sem,
    down_sem,
    mate_sem,
    left_send_sem,
    left_recv_sem,
):
    me = lax.axis_index("wide")
    rings = devices // 2
    place, core = me // 2, lax.rem(me, 2)
    mine = core * rings
    up = lax.rem(place + 1, rings) * 2 + core
    down = lax.rem(place + rings - 1, rings) * 2 + core
    mate = place * 2 + 1 - core
    owned, residues, _ = pair_ref.shape
    rows = right_ref.shape[0] // chunks
    total = left_rows.shape[1]
    width = left_rows.shape[0] // owned
    per_chunk = rows // 8
    far = rings // 2

    barrier = pltpu.get_barrier_semaphore()

    @pl.loop(1, devices)
    def _(r):
        pl.semaphore_signal(
            barrier,
            inc=1,
            device_id={"wide": lax.rem(me + r, devices)},
            device_id_type=pl.DeviceIdType.MESH,
        )

    pl.semaphore_wait(barrier, devices - 1)

    def copy(src, k, slot, sem, target):
        return pltpu.make_async_remote_copy(
            src_ref=src,
            dst_ref=held_ref.at[k * devices + slot],
            send_sem=send_sem,
            recv_sem=sem,
            device_id={"wide": target},
            device_id_type=pl.DeviceIdType.MESH,
        )

    def reach(k):
        return (far, far - 1) if k % 2 == 0 else (far - 1, far)

    def step(k, t):
        ups, downs = reach(k)
        if t == 0:
            own = right_ref.at[pl.ds(k * rows, rows)]
            slot = mine + place
            copy(own, k, slot, up_sem.at[k, 0], up).start()
            copy(own, k, slot, down_sem.at[k, 0], down).start()
            copy(own, k, slot, mate_sem.at[k], mate).start()
            return
        for sem, reached, origin, target in (
            (up_sem, ups, place + rings - t, up),
            (down_sem, downs, place + t, down),
        ):
            if t > reached:
                continue
            slot = mine + lax.rem(origin, rings)
            block = held_ref.at[k * devices + slot]
            copy(block, k, slot, sem.at[k, t - 1], target).wait_recv()
            if t < reached:
                copy(block, k, slot, sem.at[k, t], target).start()
            copy(block, k, slot, mate_sem.at[k], mate).start()

    def send_left():
        @pl.loop(1, devices)
        def _(r):
            target = lax.rem(me + r, devices)
            pltpu.make_async_remote_copy(
                src_ref=left_ref.at[target],
                dst_ref=left_held.at[mine + place],
                send_sem=left_send_sem,
                recv_sem=left_recv_sem,
                device_id={"wide": target},
                device_id_type=pl.DeviceIdType.MESH,
            ).start()

    def left_copies():
        return pltpu.make_async_remote_copy(
            src_ref=left_held.at[pl.ds(0, devices - 1)],
            dst_ref=left_held.at[pl.ds(0, devices - 1)],
            send_sem=left_send_sem,
            recv_sem=left_recv_sem,
            device_id={"wide": mate},
            device_id_type=pl.DeviceIdType.MESH,
        )

    def arrange_left():
        left_copies().wait_recv()
        left_held[mine + place] = left_ref[me]
        left_wide[...] = left_held[...].astype(F32).reshape(left_wide.shape)
        blocks = 2 * devices
        lane = lax.broadcasted_iota(jnp.int32, (blocks, total), 1)
        spread = jnp.where(
            lane // 4 == lax.broadcasted_iota(jnp.int32, (blocks, total), 0), 1.0, 0.0
        ).astype(BF16)
        column = lax.rem(lax.broadcasted_iota(jnp.int32, (width, total), 1), 4)
        for i in range(owned):
            block = left_wide[pl.ds(i, blocks, stride=owned), :].astype(BF16)
            lifted = dot_ta(block, spread)
            rows_i = lifted[:width]
            for s in range(1, 4):
                rows_i = jnp.where(column == s, lifted[s * width : (s + 1) * width], rows_i)
            left_rows[i * width : (i + 1) * width, :] = rows_i.astype(BF16)

    def arrived(k):
        theirs = held_ref.at[pl.ds(k * devices + (1 - core) * rings, rings)]
        pltpu.make_async_remote_copy(
            src_ref=theirs,
            dst_ref=theirs,
            send_sem=send_sem,
            recv_sem=mate_sem.at[k],
            device_id={"wide": mate},
            device_id_type=pl.DeviceIdType.MESH,
        ).wait_recv()
        held_ref[k * devices + mine + place] = right_ref[pl.ds(k * rows, rows), :]

    def products(k, two):
        first = slice(two * 16, two * 16 + 16)
        block = held_ref[pl.ds(k * devices, devices), first, :].astype(F32)
        for which in range(2):
            e = two * 2 + which
            right = block[:, which * 8 : which * 8 + 8, :].reshape(total, residues).astype(BF16)
            product = dot(left_rows[...], right).astype(BF16)
            y_ref[:, e * width : (e + 1) * width, :] = product.reshape(owned, width, residues)

    def project(k, start, count):
        columns = slice(k * per_chunk * width, (k + 1) * per_chunk * width)
        for i in range(start, start + count):
            part = dot(weight_ref[:, columns], y_ref[i])
            if k > 0:
                part = part + acc_ref[i]
            if k < chunks - 1:
                acc_ref[i] = part
            else:
                pair_ref[i] = part.T * (1.0 / total) + bias_ref[...]

    def pieces(k):
        yield functools.partial(arrived, k)
        for two in range(per_chunk // 2):
            yield functools.partial(products, k, two)
        for start in range(0, owned, 4):
            yield functools.partial(project, k, start, 4)

    pending = []
    last = lag * (chunks - 1) + far
    for tick in range(last + 1):
        for k in range(chunks):
            t = tick - lag * k
            if 0 <= t <= far:
                step(k, t)
                if t == far:
                    pending.extend(pieces(k))
        if tick == 0:
            send_left()
        if tick == far - 1:
            arrange_left()
        for _ in range(5):
            if pending:
                pending.pop(0)()
    for piece in pending:
        piece()
    left_copies().wait_send()
    everything = held_ref.at[pl.ds(0, chunks * (devices - 1))]
    pltpu.make_async_remote_copy(
        src_ref=everything,
        dst_ref=everything,
        send_sem=send_sem,
        recv_sem=mate_sem.at[0],
        device_id={"wide": mate},
        device_id_type=pl.DeviceIdType.MESH,
    ).wait_send()


def exchange(devices, left, right, pair_weight, pair_bias):
    _, groups, owned, _ = left.shape
    rows, residues = right.shape
    width = rows // 8
    channels = pair_weight.shape[1]
    total = devices * 8
    chunks = 4
    rings = devices // 2
    weight = jnp.transpose(pair_weight.reshape(width, width, channels), (2, 1, 0)).reshape(
        channels, width * width
    )
    whole = pl.BlockSpec(memory_space=pltpu.VMEM)
    return pl.pallas_call(
        functools.partial(exchange_kernel, devices, chunks, 2),
        in_specs=[whole] * 4,
        out_specs=whole,
        out_shape=jax.ShapeDtypeStruct((owned, residues, channels), F32),
        scratch_shapes=[
            pltpu.VMEM((chunks * devices, rows // chunks, residues), BF16),
            pltpu.VMEM((devices, groups, owned, LANES), BF16),
            pltpu.VMEM((devices * groups * owned, LANES), F32),
            pltpu.VMEM((owned * width, total), BF16),
            pltpu.VMEM((owned, (width // chunks) * width, residues), BF16),
            pltpu.VMEM((owned, channels, residues), F32),
            pltpu.SemaphoreType.DMA,
            pltpu.SemaphoreType.DMA((chunks, rings // 2)),
            pltpu.SemaphoreType.DMA((chunks, rings // 2)),
            pltpu.SemaphoreType.DMA((chunks,)),
            pltpu.SemaphoreType.DMA,
            pltpu.SemaphoreType.DMA,
        ],
        compiler_params=pltpu.CompilerParams(
            collective_id=0, has_side_effects=True, vmem_limit_bytes=48 << 20
        ),
        cost_estimate=pl.CostEstimate(
            flops=7_000_000_000, bytes_accessed=12 << 20, transcendentals=0
        ),
        name="exchange_outer",
    )(left, right, weight, pair_bias[None, :])


def shards(
    alignment_token_ids,
    residue_index_offsets,
    target_residue_feature,
    token_embedding_table,
    attention_norm_gain,
    query_weight,
    key_weight,
    value_weight,
    gate_weight,
    gate_offset_bias,
    output_weight,
    relative_position_table,
    product_norm_gain,
    left_weight,
    right_weight,
    pair_weight,
    pair_projection_bias,
):
    devices = lax.axis_size("wide")
    updated, left, right = attention(
        devices,
        alignment_token_ids,
        residue_index_offsets,
        target_residue_feature,
        token_embedding_table,
        attention_norm_gain,
        query_weight,
        key_weight,
        value_weight,
        gate_weight,
        gate_offset_bias,
        output_weight,
        relative_position_table,
        product_norm_gain,
        left_weight,
        right_weight,
    )
    pair = exchange(devices, left, right, pair_weight, pair_projection_bias)
    return (updated, pair)


def solution(mesh):
    placed = (
        P(("groups", "wide"), None),
        P("groups"),
        P("groups", None),
    ) + (P(),) * 14
    return jax.shard_map(
        shards,
        mesh=mesh,
        in_specs=placed,
        out_specs=(P(("groups", "wide"), None, None), P(("groups", "wide"), None, None)),
        check_vma=False,
    )
```

```python
import functools

import jax
import jax.numpy as jnp
from jax import lax
from jax.experimental import pallas as pl
from jax.experimental.pallas import tpu as pltpu
from jax.sharding import PartitionSpec as P

REACH = 32
LANES = 128
F32 = jnp.float32
BF16 = jnp.bfloat16


def dot(a, b):
    return lax.dot_general(a, b, (((1,), (0,)), ((), ())), preferred_element_type=F32)


def dot_tb(a, b):
    return lax.dot_general(a, b, (((1,), (1,)), ((), ())), preferred_element_type=F32)


def dot_ta(a, b):
    return lax.dot_general(a, b, (((0,), (0,)), ((), ())), preferred_element_type=F32)


def layer_normalize(values, gain):
    center = jnp.mean(values, axis=-1, keepdims=True)
    centred = values - center
    spread = jnp.mean(centred * centred, axis=-1, keepdims=True)
    return centred * lax.rsqrt(spread + 1e-05) * gain


GROUPS = 2
CHUNKS = 4
STARTS = (0, 0, 1, 1)


def block_kernel(
    devices,
    heads,
    tok_ref,
    pos_row_ref,
    target_ref,
    emb_ref,
    gain_one_ref,
    wq_ref,
    wk_ref,
    wv_ref,
    wg_ref,
    gb_ref,
    wo_ref,
    table_ref,
    gain_two_ref,
    wl_ref,
    wr_ref,
    raw_weight_ref,
    pair_bias_ref,
    au_ref,
    pair_ref,
    bias_ref,
    turn_ref,
    wl4_ref,
    wr4_ref,
    wide_weight,
    weight_ref,
    emb3_ref,
    score_ref,
    prob_ref,
    mixed_ref,
    left_acc,
    right_acc,
    left_out,
    left_held,
    left_wide,
    left_rows,
    held_ref,
    y_ref,
    acc_ref,
    send_sem,
    up_sem,
    down_sem,
    mate_sem,
    left_send_sem,
    left_recv_sem,
):
    seq = pl.program_id(0)
    sequences = tok_ref.shape[0]
    share = sequences // GROUPS
    residues, features = target_ref.shape
    classes = emb_ref.shape[0]
    head_size = features // heads
    per_half = LANES // head_size
    owned = pair_ref.shape[0]
    width = right_acc.shape[1] // sequences
    group_rows = width * share
    rows = group_rows // CHUNKS
    total = left_rows.shape[2]
    per_chunk = width // CHUNKS

    me = lax.axis_index("wide")
    rings = devices // 2
    place, core = me // 2, lax.rem(me, 2)
    mine = core * rings
    up = lax.rem(place + 1, rings) * 2 + core
    down = lax.rem(place + rings - 1, rings) * 2 + core
    mate = place * 2 + 1 - core
    far = rings // 2
    swap = lax.rem(place, 2) * 2

    barrier = pltpu.get_barrier_semaphore()

    @pl.when(seq == 0)
    def _():
        @pl.loop(1, devices)
        def _(r):
            pl.semaphore_signal(
                barrier,
                inc=1,
                device_id={"wide": lax.rem(me + r, devices)},
                device_id_type=pl.DeviceIdType.MESH,
            )

    @pl.when(seq == share - 1)
    def _():
        pl.semaphore_wait(barrier, devices - 1)

    def remote(src, dst, send, recv, target):
        return pltpu.make_async_remote_copy(
            src_ref=src,
            dst_ref=dst,
            send_sem=send,
            recv_sem=recv,
            device_id={"wide": target},
            device_id_type=pl.DeviceIdType.MESH,
        )

    def reach(k):
        return (far, far - 1) if k % 2 == 0 else (far - 1, far)

    def step(g, k, t):
        base = (g * CHUNKS + k) * devices
        which = g * CHUNKS + k
        ups, downs = reach(k)

        def begin():
            own = held_ref.at[base + mine + place]
            remote(own, own, send_sem, up_sem.at[which, 0], up).start()
            remote(own, own, send_sem, down_sem.at[which, 0], down).start()
            remote(own, own, send_sem, mate_sem.at[which], mate).start()

        def forward():
            for sem, reached, origin, target in (
                (up_sem, ups, place + rings - t, up),
                (down_sem, downs, place + t, down),
            ):
                if isinstance(t, int) and t > reached:
                    continue
                item = held_ref.at[base + mine + lax.rem(origin, rings)]
                remote(item, item, send_sem, sem.at[which, t - 1], target).wait_recv()

                def onward(item=item, sem=sem, target=target):
                    remote(item, item, send_sem, sem.at[which, t], target).start()
                if not isinstance(t, int):
                    pl.when(t < reached)(onward)
                elif t < reached:
                    onward()
                remote(item, item, send_sem, mate_sem.at[which], mate).start()

        if isinstance(t, int):
            begin() if t == 0 else forward()
        else:
            pl.when(t == 0)(begin)
            pl.when(t > 0)(forward)

    def send_left(g):
        @pl.loop(1, devices)
        def _(r):
            target = lax.rem(me + r, devices)
            remote(
                left_out.at[g * devices + target],
                left_held.at[g * devices + mine + place],
                left_send_sem,
                left_recv_sem.at[g],
                target,
            ).start()

    def ring_slot(slot):
        @pl.when(seq >= share)
        def _():
            t = (seq - share) * 2 + slot // 2
            for k in range(CHUNKS):
                if k // 2 == slot % 2:
                    step(0, k, t)
            if slot == 0:
                pl.when(seq == share)(functools.partial(send_left, 0))

    @pl.when(seq == 0)
    def _():
        turn_ref[...] = jnp.zeros_like(turn_ref)
        turn_ref[:, : table_ref.shape[1]] = table_ref[...]
        table_rows = turn_ref[...]
        spots = pos_row_ref[...].astype(F32)
        tiles = residues // LANES
        for tile in range(tiles):
            cols = slice(tile * LANES, (tile + 1) * LANES)
            across = jnp.broadcast_to(spots[:, cols], (LANES, LANES))
            down_rows = across.T
            for sub in range(LANES // REACH):
                span = slice(tile * LANES + sub * REACH, tile * LANES + (sub + 1) * REACH)
                own = down_rows[sub * REACH : (sub + 1) * REACH, :]
                for other in range(tiles):
                    dst = slice(other * LANES, (other + 1) * LANES)
                    near = (
                        other == tile
                        or (other == tile - 1 and sub == 0)
                        or (other == tile + 1 and sub == LANES // REACH - 1)
                    )
                    if near:
                        delta = jnp.broadcast_to(spots[:, dst], (REACH, LANES)) - own
                        offs = (jnp.clip(delta, -REACH, REACH) + REACH).astype(jnp.int32)
                    for h in range(heads):
                        row = table_rows[h : h + 1, :]
                        if near:
                            bias_ref[h, span, dst] = jnp.take_along_axis(
                                jnp.broadcast_to(row, (REACH, LANES)),
                                offs,
                                axis=1,
                                mode="promise_in_bounds",
                            )
                        else:
                            edge = row[:, 2 * REACH : 2 * REACH + 1] if other > tile else row[:, :1]
                            bias_ref[h, span, dst] = jnp.broadcast_to(edge, (REACH, LANES))

        wl4_ref[...] = jnp.zeros_like(wl4_ref)
        for k in range(share):
            wl4_ref[k, k * width : (k + 1) * width, :] = wl_ref[...]
        for col in range(features // LANES):
            wr4_ref[0, col] = wr_ref[:, col * LANES : (col + 1) * LANES].astype(F32)
        for x in range(1, 4):
            for p in range(4):
                for col in range(features // LANES):
                    wr4_ref[x, col, pl.ds(p, width // 4, stride=4), :] = wr4_ref[
                        0, col, pl.ds(p ^ x, width // 4, stride=4), :
                    ]

        emb3_ref[...] = jnp.zeros_like(emb3_ref)
        rest = emb_ref[...]
        for part in range(3):
            piece = rest.astype(BF16)
            emb3_ref[part * 32 : part * 32 + classes, :] = piece
            rest = rest - piece.astype(F32)
        left_acc[...] = jnp.zeros_like(left_acc)

    token = tok_ref[pl.ds(seq, 1), :]
    klass = lax.broadcasted_iota(jnp.int32, (LANES, residues), 0)
    onehot = jnp.where((klass % 32 == token) & (klass < 96), 1.0, 0.0).astype(BF16)
    start = dot_ta(onehot, emb3_ref[...]) + target_ref[...]
    normed = layer_normalize(start, gain_one_ref[...]).astype(BF16)
    query = (dot(normed, wq_ref[...]) * (1.0 / head_size**0.5)).astype(BF16)
    keys = dot(normed, wk_ref[...]).astype(BF16)
    values = dot(normed, wv_ref[...]).astype(BF16)
    lane = lax.broadcasted_iota(jnp.int32, (residues, features), 1) // head_size
    half_lane = lax.broadcasted_iota(jnp.int32, (residues, LANES), 1) // head_size
    ones = jnp.ones((residues, LANES), BF16)

    def score(h):
        masked = jnp.where(lane == h, query, jnp.zeros_like(query))
        score_ref[h % 4] = dot_tb(masked, keys)

    def soften(h):
        for piece in range(residues // LANES):
            span = slice(piece * LANES, (piece + 1) * LANES)
            scores = score_ref[h % 4, span, :] + bias_ref[h, span, :]
            peak = jnp.max(scores, axis=1, keepdims=True)
            prob_ref[h % 4, span, :] = jnp.exp(scores - peak).astype(BF16)

    def mix(h):
        half, spot = divmod(h, per_half)
        cols = slice(half * LANES, (half + 1) * LANES)
        product = dot(prob_ref[h % 4], jnp.concatenate([values[:, cols], ones], axis=1))
        result = product[:, :LANES] / product[:, LANES:]
        if spot == 0:
            mixed_ref[:, cols] = result
        else:
            mixed_ref[:, cols] = jnp.where(half_lane == spot, result, mixed_ref[:, cols])

    stages = heads // 2
    score(0)
    score(1)
    for stage in range(stages):
        for which in range(2):
            if stage + 1 < stages:
                score(stage * 2 + 2 + which)
            soften(stage * 2 + which)
            if stage > 0:
                mix(stage * 2 - 2 + which)
        ring_slot(stage)
    mix(heads - 2)
    mix(heads - 1)

    gate = jax.nn.sigmoid(dot(normed, wg_ref[...]) + gb_ref[...])
    mixed = (mixed_ref[...] * gate).astype(BF16)
    updated = start + dot(mixed, wo_ref[...])
    au_ref[0] = updated
    second = layer_normalize(updated, gain_two_ref[...]).astype(BF16)
    group = seq // share
    member = lax.rem(seq, share)
    span = pl.ds(pl.multiple_of(group * residues, residues), residues)
    left_acc[span, :] += dot_tb(second, wl4_ref[member])
    parts = [wr4_ref[swap + group, col] for col in range(features // LANES)]
    right = dot_tb(jnp.concatenate(parts, axis=1).astype(BF16), second)
    for col in range(residues // LANES):
        right_acc[col, pl.ds(group * group_rows + member, width, stride=share), :] = right[
            :, col * LANES : (col + 1) * LANES
        ]

    def finish_group(g):
        part = left_acc[g * residues : (g + 1) * residues, :].astype(BF16)
        left_out[g * devices : (g + 1) * devices] = part.reshape(devices, owned, LANES)
        for k in range(CHUNKS):
            first = g * group_rows + k * rows
            for col in range(residues // LANES):
                held_ref[
                    (g * CHUNKS + k) * devices + mine + place,
                    :,
                    col * LANES : (col + 1) * LANES,
                ] = right_acc[col, first : first + rows, :].astype(BF16)

    for g in range(GROUPS):
        pl.when(seq == (g + 1) * share - 1)(functools.partial(finish_group, g))

    def arrange_left():
        for g in range(GROUPS):
            arrived = left_held.at[pl.ds(g * devices, devices - 1)]
            remote(arrived, arrived, left_send_sem, left_recv_sem.at[g], mate).wait_recv()
            left_held[g * devices + mine + place] = left_out[g * devices + me]
        left_wide[...] = left_held[...].astype(F32).reshape(left_wide.shape)
        blocks = GROUPS * devices
        block_id = lax.broadcasted_iota(jnp.int32, (blocks, total), 0)
        lane_id = lax.broadcasted_iota(jnp.int32, (blocks, total), 1)
        column = lax.rem(lax.broadcasted_iota(jnp.int32, (width, total), 1), share)
        spreads = []
        for pattern in range(4):
            high = lax.rem(lane_id // 8, 2) ^ (pattern // 2)
            low = lax.rem(lane_id // 4, 2) ^ (pattern % 2)
            origin = low * devices + lane_id // 16 * 2 + high
            spreads.append(jnp.where(origin == block_id, 1.0, 0.0).astype(BF16))
        for i in range(owned):
            piece = left_wide[pl.ds(i, blocks, stride=owned), :].astype(BF16)
            for pattern in range(4):
                lifted = dot_ta(piece, spreads[pattern])
                chosen = lifted[:width]
                for s in range(1, share):
                    chosen = jnp.where(column == s, lifted[s * width : (s + 1) * width], chosen)
                left_rows[pattern, i * width : (i + 1) * width, :] = chosen.astype(BF16)

    def turn_weight():
        wide_weight[...] = raw_weight_ref[...].astype(F32)
        for k in range(CHUNKS):
            strips = [
                wide_weight[pl.ds(k * per_chunk + e, width, stride=width), :]
                for e in range(per_chunk)
            ]
            columns = slice(k * per_chunk * width, (k + 1) * per_chunk * width)
            weight_ref[:, columns] = jnp.concatenate(strips, axis=0).T.astype(BF16)

    def arrived(k):
        for g in range(GROUPS):
            which = g * CHUNKS + k
            theirs = held_ref.at[pl.ds(which * devices + (1 - core) * rings, rings)]
            remote(theirs, theirs, send_sem, mate_sem.at[which], mate).wait_recv()

    def products(k, quad, col):
        first = slice(quad * 16, quad * 16 + 16)
        cols = slice(col * 256, (col + 1) * 256)
        one, two = (
            held_ref[(g * CHUNKS + k) * devices : (g * CHUNKS + k + 1) * devices, first, cols]
            for g in range(GROUPS)
        )
        row = lax.broadcasted_iota(jnp.int32, one.shape, 1)
        even = lax.rem(row // 4, 2) == 0
        half = devices // 2
        upper = lax.broadcasted_iota(jnp.int32, (half,) + one.shape[1:], 1) < 8
        for low in range(2):
            picked = jnp.where(even, one, two) if low == 0 else jnp.where(even, two, one)
            picked = picked.reshape((half, 2) + one.shape[1:])
            evens, odds = picked[:, 0], picked[:, 1]
            for high in range(2):
                pattern = high * 2 + low
                e = quad * 4 + pattern
                right = jnp.where(upper, evens, odds) if high == 0 else jnp.where(upper, odds, evens)
                product = dot(left_rows[pattern], right.reshape(total, 256)).astype(BF16)
                y_ref[:, e * width : (e + 1) * width, cols] = product.reshape(owned, width, 256)

    def project(k, begin, count):
        columns = slice(k * per_chunk * width, (k + 1) * per_chunk * width)
        for i in range(begin, begin + count):
            part = dot(weight_ref[:, columns], y_ref[i])
            if k > 0:
                part = part + acc_ref[i]
            if k < CHUNKS - 1:
                acc_ref[i] = part
            else:
                pair_ref[i] = part.T * (1.0 / total) + pair_bias_ref[...]

    def pieces(k):
        yield functools.partial(arrived, k)
        for quad in range(per_chunk // 4):
            for col in range(residues // 256):
                yield functools.partial(products, k, quad, col)
        for begin in range(0, owned, 4):
            yield functools.partial(project, k, begin, 4)

    @pl.when(seq == sequences - 1)
    def _():
        pending = []
        last = max(STARTS) + far
        for tick in range(last + 1):
            for k in range(CHUNKS):
                t = tick - STARTS[k]
                if 0 <= t <= far:
                    step(1, k, t)
                    if t == far:
                        pending.extend(pieces(k))
                if tick == 0:
                    step(0, k, far)
            if tick == 0:
                send_left(1)
            if tick == 1:
                turn_weight()
            if tick == far - 2:
                arrange_left()
            for _ in range(5):
                if pending:
                    pending.pop(0)()
        for piece in pending:
            piece()
        sent = left_held.at[pl.ds(0, GROUPS * (devices - 1))]
        remote(sent, sent, left_send_sem, left_recv_sem.at[0], mate).wait_send()
        everything = held_ref.at[pl.ds(0, GROUPS * CHUNKS * (devices - 1))]
        remote(everything, everything, send_sem, mate_sem.at[0], mate).wait_send()


def block(
    devices,
    tokens,
    positions,
    target,
    emb,
    gain_one,
    wq,
    wk,
    wv,
    wg,
    gb,
    wo,
    table,
    gain_two,
    wl,
    wr,
    pair_weight,
    pair_bias,
):
    sequences, residues = tokens.shape
    features = target.shape[1]
    heads = table.shape[1]
    width = wl.shape[1]
    channels = pair_weight.shape[1]
    owned = residues // devices
    rings = devices // 2
    total = devices * sequences
    share = sequences // GROUPS
    operands = (
        tokens,
        positions[None, :],
        target,
        emb,
        gain_one[None, :],
        wq,
        wk,
        wv,
        wg,
        gb[None, :],
        wo,
        table.T,
        gain_two[None, :],
        wl.T,
        wr.T,
        pair_weight,
        pair_bias[None, :],
    )

    def const(a):
        return pl.BlockSpec(
            a.shape, lambda s: (0,) * a.ndim, pipeline_mode=pl.Buffered(buffer_count=1)
        )

    return pl.pallas_call(
        functools.partial(block_kernel, devices, heads),
        grid=(sequences,),
        in_specs=[const(a) for a in operands],
        out_specs=(
            pl.BlockSpec((1, residues, features), lambda s: (s, 0, 0)),
            pl.BlockSpec(memory_space=pltpu.VMEM),
        ),
        out_shape=(
            jax.ShapeDtypeStruct((sequences, residues, features), F32),
            jax.ShapeDtypeStruct((owned, residues, channels), F32),
        ),
        scratch_shapes=[
            pltpu.VMEM((heads, residues, residues), F32),
            pltpu.VMEM((heads, LANES), F32),
            pltpu.VMEM((share, LANES, features), BF16),
            pltpu.VMEM((4, features // LANES, width, LANES), F32),
            pltpu.VMEM((width * width, channels), F32),
            pltpu.VMEM((channels, width * width), BF16),
            pltpu.VMEM((LANES, features), BF16),
            pltpu.VMEM((4, residues, residues), F32),
            pltpu.VMEM((4, residues, residues), BF16),
            pltpu.VMEM((residues, features), F32),
            pltpu.VMEM((GROUPS * residues, LANES), F32),
            pltpu.VMEM((residues // LANES, width * sequences, LANES), F32),
            pltpu.VMEM((GROUPS * devices, owned, LANES), BF16),
            pltpu.VMEM((GROUPS * devices, owned, LANES), BF16),
            pltpu.VMEM((GROUPS * devices * owned, LANES), F32),
            pltpu.VMEM((4, owned * width, total), BF16),
            pltpu.VMEM((GROUPS * CHUNKS * devices, width * share // CHUNKS, residues), BF16),
            pltpu.VMEM((owned, (width // CHUNKS) * width, residues), BF16),
            pltpu.VMEM((owned, channels, residues), F32),
            pltpu.SemaphoreType.DMA,
            pltpu.SemaphoreType.DMA((GROUPS * CHUNKS, rings // 2)),
            pltpu.SemaphoreType.DMA((GROUPS * CHUNKS, rings // 2)),
            pltpu.SemaphoreType.DMA((GROUPS * CHUNKS,)),
            pltpu.SemaphoreType.DMA,
            pltpu.SemaphoreType.DMA((GROUPS,)),
        ],
        compiler_params=pltpu.CompilerParams(
            dimension_semantics=("arbitrary",),
            collective_id=0,
            has_side_effects=True,
            vmem_limit_bytes=60 << 20,
        ),
        cost_estimate=pl.CostEstimate(
            flops=27_000_000_000, bytes_accessed=14 << 20, transcendentals=17_000_000
        ),
        name="msa_block",
    )(*operands)


def shards(
    alignment_token_ids,
    residue_index_offsets,
    target_residue_feature,
    token_embedding_table,
    attention_norm_gain,
    query_weight,
    key_weight,
    value_weight,
    gate_weight,
    gate_offset_bias,
    output_weight,
    relative_position_table,
    product_norm_gain,
    left_weight,
    right_weight,
    pair_weight,
    pair_projection_bias,
):
    return block(
        lax.axis_size("wide"),
        alignment_token_ids,
        residue_index_offsets,
        target_residue_feature,
        token_embedding_table,
        attention_norm_gain,
        query_weight,
        key_weight,
        value_weight,
        gate_weight,
        gate_offset_bias,
        output_weight,
        relative_position_table,
        product_norm_gain,
        left_weight,
        right_weight,
        pair_weight,
        pair_projection_bias,
    )


def solution(mesh):
    placed = (
        P(("groups", "wide"), None),
        P("groups"),
        P("groups", None),
    ) + (P(),) * 14
    return jax.shard_map(
        shards,
        mesh=mesh,
        in_specs=placed,
        out_specs=(P(("groups", "wide"), None, None), P(("groups", "wide"), None, None)),
        check_vma=False,
    )
```

```python
import functools

import jax
import jax.numpy as jnp
from jax import lax
from jax.experimental import pallas as pl
from jax.experimental.pallas import tpu as pltpu
from jax.sharding import PartitionSpec as P

REACH = 32
LANES = 128
F32 = jnp.float32
BF16 = jnp.bfloat16


def dot(a, b):
    return lax.dot_general(a, b, (((1,), (0,)), ((), ())), preferred_element_type=F32)


def dot_tb(a, b):
    return lax.dot_general(a, b, (((1,), (1,)), ((), ())), preferred_element_type=F32)


def dot_ta(a, b):
    return lax.dot_general(a, b, (((0,), (0,)), ((), ())), preferred_element_type=F32)


def layer_normalize(values, gain):
    center = jnp.mean(values, axis=-1, keepdims=True)
    centred = values - center
    spread = jnp.mean(centred * centred, axis=-1, keepdims=True)
    return centred * lax.rsqrt(spread + 1e-05) * gain


GROUPS = 2
CHUNKS = 4
STARTS = (0, 0, 1, 1)


def block_kernel(
    devices,
    heads,
    tok_ref,
    pos_row_ref,
    target_ref,
    emb_ref,
    gain_one_ref,
    wq_ref,
    wk_ref,
    wv_ref,
    wg_ref,
    gb_ref,
    wo_ref,
    table_ref,
    gain_two_ref,
    wl_ref,
    wr_ref,
    raw_weight_ref,
    pair_bias_ref,
    au_ref,
    pair_ref,
    bias_ref,
    turn_ref,
    wl4_ref,
    wr4_ref,
    wide_weight,
    weight_ref,
    emb3_ref,
    score_ref,
    prob_ref,
    mixed_ref,
    left_acc,
    right_acc,
    left_out,
    left_held,
    left_wide,
    left_rows,
    held_ref,
    y_ref,
    acc_ref,
    send_sem,
    up_sem,
    down_sem,
    mate_sem,
    left_send_sem,
    left_recv_sem,
):
    seq = pl.program_id(0)
    sequences = tok_ref.shape[0]
    share = sequences // GROUPS
    residues, features = target_ref.shape
    classes = emb_ref.shape[0]
    head_size = features // heads
    per_half = LANES // head_size
    owned = pair_ref.shape[0]
    width = right_acc.shape[1] // sequences
    group_rows = width * share
    rows = group_rows // CHUNKS
    total = left_rows.shape[2]
    per_chunk = width // CHUNKS

    me = lax.axis_index("wide")
    rings = devices // 2
    place, core = me // 2, lax.rem(me, 2)
    mine = core * rings
    up = lax.rem(place + 1, rings) * 2 + core
    down = lax.rem(place + rings - 1, rings) * 2 + core
    mate = place * 2 + 1 - core
    far = rings // 2
    swap = lax.rem(place, 2) * 2

    barrier = pltpu.get_barrier_semaphore()

    @pl.when(seq == 0)
    def _():
        @pl.loop(1, devices)
        def _(r):
            pl.semaphore_signal(
                barrier,
                inc=1,
                device_id={"wide": lax.rem(me + r, devices)},
                device_id_type=pl.DeviceIdType.MESH,
            )

    @pl.when(seq == share - 1)
    def _():
        pl.semaphore_wait(barrier, devices - 1)

    def remote(src, dst, send, recv, target):
        return pltpu.make_async_remote_copy(
            src_ref=src,
            dst_ref=dst,
            send_sem=send,
            recv_sem=recv,
            device_id={"wide": target},
            device_id_type=pl.DeviceIdType.MESH,
        )

    def reach(k):
        return (far, far - 1) if k % 2 == 0 else (far - 1, far)

    def step(g, k, t):
        base = (g * CHUNKS + k) * devices
        which = g * CHUNKS + k
        ups, downs = reach(k)

        def begin():
            own = held_ref.at[base + mine + place]
            remote(own, own, send_sem, up_sem.at[which, 0], up).start()
            remote(own, own, send_sem, down_sem.at[which, 0], down).start()
            remote(own, own, send_sem, mate_sem.at[which], mate).start()

        def forward():
            for sem, reached, origin, target in (
                (up_sem, ups, place + rings - t, up),
                (down_sem, downs, place + t, down),
            ):
                if isinstance(t, int) and t > reached:
                    continue
                item = held_ref.at[base + mine + lax.rem(origin, rings)]
                remote(item, item, send_sem, sem.at[which, t - 1], target).wait_recv()

                def onward(item=item, sem=sem, target=target):
                    remote(item, item, send_sem, sem.at[which, t], target).start()
                if not isinstance(t, int):
                    pl.when(t < reached)(onward)
                elif t < reached:
                    onward()
                remote(item, item, send_sem, mate_sem.at[which], mate).start()

        if isinstance(t, int):
            begin() if t == 0 else forward()
        else:
            pl.when(t == 0)(begin)
            pl.when(t > 0)(forward)

    def send_left_to(g, r):
        target = lax.rem(me + r, devices)
        remote(
            left_out.at[g * devices + target],
            left_held.at[g * devices + mine + place],
            left_send_sem,
            left_recv_sem.at[g],
            target,
        ).start()

    def send_left(g):
        @pl.loop(1, devices)
        def _(r):
            send_left_to(g, r)

    def ring_slot(slot):
        @pl.when(seq >= share)
        def _():
            t = (seq - share) * 2 + slot // 2
            for k in range(CHUNKS):
                if k // 2 == slot % 2:
                    step(0, k, t)
            each = pl.cdiv(devices - 1, 4 * share)
            first = ((seq - share) * 4 + slot) * each + 1
            for r in range(each):
                pl.when(first + r < devices)(functools.partial(send_left_to, 0, first + r))

    @pl.when(seq == 0)
    def _():
        turn_ref[...] = jnp.zeros_like(turn_ref)
        turn_ref[:, : table_ref.shape[1]] = table_ref[...]
        table_rows = turn_ref[...]
        spots = pos_row_ref[...].astype(F32)
        tiles = residues // LANES
        for tile in range(tiles):
            cols = slice(tile * LANES, (tile + 1) * LANES)
            across = jnp.broadcast_to(spots[:, cols], (LANES, LANES))
            down_rows = across.T
            for sub in range(LANES // REACH):
                span = slice(tile * LANES + sub * REACH, tile * LANES + (sub + 1) * REACH)
                own = down_rows[sub * REACH : (sub + 1) * REACH, :]
                for other in range(tiles):
                    dst = slice(other * LANES, (other + 1) * LANES)
                    near = (
                        other == tile
                        or (other == tile - 1 and sub == 0)
                        or (other == tile + 1 and sub == LANES // REACH - 1)
                    )
                    if near:
                        delta = jnp.broadcast_to(spots[:, dst], (REACH, LANES)) - own
                        offs = (jnp.clip(delta, -REACH, REACH) + REACH).astype(jnp.int32)
                    for h in range(heads):
                        row = table_rows[h : h + 1, :]
                        if near:
                            bias_ref[h, span, dst] = jnp.take_along_axis(
                                jnp.broadcast_to(row, (REACH, LANES)),
                                offs,
                                axis=1,
                                mode="promise_in_bounds",
                            )
                        else:
                            edge = row[:, 2 * REACH : 2 * REACH + 1] if other > tile else row[:, :1]
                            bias_ref[h, span, dst] = jnp.broadcast_to(edge, (REACH, LANES))

        wl4_ref[...] = jnp.zeros_like(wl4_ref)
        for k in range(share):
            wl4_ref[k, k * width : (k + 1) * width, :] = wl_ref[...]
        for col in range(features // LANES):
            wr4_ref[0, col] = wr_ref[:, col * LANES : (col + 1) * LANES].astype(F32)
        for x in range(1, 4):
            for p in range(4):
                for col in range(features // LANES):
                    wr4_ref[x, col, pl.ds(p, width // 4, stride=4), :] = wr4_ref[
                        0, col, pl.ds(p ^ x, width // 4, stride=4), :
                    ]

        emb3_ref[...] = jnp.zeros_like(emb3_ref)
        rest = emb_ref[...]
        for part in range(3):
            piece = rest.astype(BF16)
            emb3_ref[part * 32 : part * 32 + classes, :] = piece
            rest = rest - piece.astype(F32)
        left_acc[...] = jnp.zeros_like(left_acc)

    token = tok_ref[pl.ds(seq, 1), :]
    klass = lax.broadcasted_iota(jnp.int32, (LANES, residues), 0)
    onehot = jnp.where((klass % 32 == token) & (klass < 96), 1.0, 0.0).astype(BF16)
    start = dot_ta(onehot, emb3_ref[...]) + target_ref[...]
    normed = layer_normalize(start, gain_one_ref[...]).astype(BF16)
    query = (dot(normed, wq_ref[...]) * (1.0 / head_size**0.5)).astype(BF16)
    keys = dot(normed, wk_ref[...]).astype(BF16)
    values = dot(normed, wv_ref[...]).astype(BF16)
    lane = lax.broadcasted_iota(jnp.int32, (residues, features), 1) // head_size
    half_lane = lax.broadcasted_iota(jnp.int32, (residues, LANES), 1) // head_size
    ones = jnp.ones((residues, LANES), BF16)

    def score(h):
        masked = jnp.where(lane == h, query, jnp.zeros_like(query))
        score_ref[h % 4] = dot_tb(masked, keys)

    def soften(h):
        for piece in range(residues // LANES):
            span = slice(piece * LANES, (piece + 1) * LANES)
            scores = score_ref[h % 4, span, :] + bias_ref[h, span, :]
            peak = jnp.max(scores, axis=1, keepdims=True)
            prob_ref[h % 4, span, :] = jnp.exp(scores - peak).astype(BF16)

    def mix(h):
        half, spot = divmod(h, per_half)
        cols = slice(half * LANES, (half + 1) * LANES)
        product = dot(prob_ref[h % 4], jnp.concatenate([values[:, cols], ones], axis=1))
        result = product[:, :LANES] / product[:, LANES:]
        if spot == 0:
            mixed_ref[:, cols] = result
        else:
            mixed_ref[:, cols] = jnp.where(half_lane == spot, result, mixed_ref[:, cols])

    stages = heads // 2
    slots = {0: 0, 1: 1, stages - 1: 2}
    score(0)
    score(1)
    for stage in range(stages):
        for which in range(2):
            if stage + 1 < stages:
                score(stage * 2 + 2 + which)
            soften(stage * 2 + which)
            if stage > 0:
                mix(stage * 2 - 2 + which)
        if stage in slots:
            ring_slot(slots[stage])
    mix(heads - 2)
    mix(heads - 1)

    gate = jax.nn.sigmoid(dot(normed, wg_ref[...]) + gb_ref[...])
    mixed = (mixed_ref[...] * gate).astype(BF16)
    updated = start + dot(mixed, wo_ref[...])
    au_ref[0] = updated
    ring_slot(3)
    second = layer_normalize(updated, gain_two_ref[...]).astype(BF16)
    group = seq // share
    member = lax.rem(seq, share)
    span = pl.ds(pl.multiple_of(group * residues, residues), residues)
    left_acc[span, :] += dot_tb(second, wl4_ref[member])
    parts = [wr4_ref[swap + group, col] for col in range(features // LANES)]
    right = dot_tb(jnp.concatenate(parts, axis=1).astype(BF16), second)
    for col in range(residues // LANES):
        right_acc[col, pl.ds(group * group_rows + member, width, stride=share), :] = right[
            :, col * LANES : (col + 1) * LANES
        ]

    def finish_group(g):
        part = left_acc[g * residues : (g + 1) * residues, :].astype(BF16)
        left_out[g * devices : (g + 1) * devices] = part.reshape(devices, owned, LANES)
        for k in range(CHUNKS):
            first = g * group_rows + k * rows
            for col in range(residues // LANES):
                held_ref[
                    (g * CHUNKS + k) * devices + mine + place,
                    :,
                    col * LANES : (col + 1) * LANES,
                ] = right_acc[col, first : first + rows, :].astype(BF16)

    for g in range(GROUPS):
        pl.when(seq == (g + 1) * share - 1)(functools.partial(finish_group, g))

    def arrange_left():
        for g in range(GROUPS):
            arrived = left_held.at[pl.ds(g * devices, devices - 1)]
            remote(arrived, arrived, left_send_sem, left_recv_sem.at[g], mate).wait_recv()
            left_held[g * devices + mine + place] = left_out[g * devices + me]
        left_wide[...] = left_held[...].astype(F32).reshape(left_wide.shape)
        blocks = GROUPS * devices
        block_id = lax.broadcasted_iota(jnp.int32, (blocks, total), 0)
        lane_id = lax.broadcasted_iota(jnp.int32, (blocks, total), 1)
        column = lax.rem(lax.broadcasted_iota(jnp.int32, (width, total), 1), share)
        spreads = []
        for pattern in range(4):
            high = lax.rem(lane_id // 8, 2) ^ (pattern // 2)
            low = lax.rem(lane_id // 4, 2) ^ (pattern % 2)
            origin = low * devices + lane_id // 16 * 2 + high
            spreads.append(jnp.where(origin == block_id, 1.0, 0.0).astype(BF16))
        for i in range(owned):
            piece = left_wide[pl.ds(i, blocks, stride=owned), :].astype(BF16)
            for pattern in range(4):
                lifted = dot_ta(piece, spreads[pattern])
                chosen = lifted[:width]
                for s in range(1, share):
                    chosen = jnp.where(column == s, lifted[s * width : (s + 1) * width], chosen)
                left_rows[pattern, i * width : (i + 1) * width, :] = chosen.astype(BF16)

    def turn_weight():
        wide_weight[...] = raw_weight_ref[...].astype(F32)
        for k in range(CHUNKS):
            strips = [
                wide_weight[pl.ds(k * per_chunk + e, width, stride=width), :]
                for e in range(per_chunk)
            ]
            columns = slice(k * per_chunk * width, (k + 1) * per_chunk * width)
            weight_ref[:, columns] = jnp.concatenate(strips, axis=0).T.astype(BF16)

    def arrived(k):
        for g in range(GROUPS):
            which = g * CHUNKS + k
            theirs = held_ref.at[pl.ds(which * devices + (1 - core) * rings, rings)]
            remote(theirs, theirs, send_sem, mate_sem.at[which], mate).wait_recv()

    def products(k, quad, col):
        first = slice(quad * 16, quad * 16 + 16)
        cols = slice(col * 256, (col + 1) * 256)
        one, two = (
            held_ref[(g * CHUNKS + k) * devices : (g * CHUNKS + k + 1) * devices, first, cols]
            for g in range(GROUPS)
        )
        row = lax.broadcasted_iota(jnp.int32, one.shape, 1)
        even = lax.rem(row // 4, 2) == 0
        half = devices // 2
        upper = lax.broadcasted_iota(jnp.int32, (half,) + one.shape[1:], 1) < 8
        for low in range(2):
            picked = jnp.where(even, one, two) if low == 0 else jnp.where(even, two, one)
            picked = picked.reshape((half, 2) + one.shape[1:])
            evens, odds = picked[:, 0], picked[:, 1]
            for high in range(2):
                pattern = high * 2 + low
                e = quad * 4 + pattern
                right = jnp.where(upper, evens, odds) if high == 0 else jnp.where(upper, odds, evens)
                product = dot(left_rows[pattern], right.reshape(total, 256)).astype(BF16)
                y_ref[:, e * width : (e + 1) * width, cols] = product.reshape(owned, width, 256)

    def project(k, begin, count):
        columns = slice(k * per_chunk * width, (k + 1) * per_chunk * width)
        for i in range(begin, begin + count):
            part = dot(weight_ref[:, columns], y_ref[i])
            if k > 0:
                part = part + acc_ref[i]
            if k < CHUNKS - 1:
                acc_ref[i] = part
            else:
                pair_ref[i] = part.T * (1.0 / total) + pair_bias_ref[...]

    def pieces(k):
        yield functools.partial(arrived, k)
        for quad in range(per_chunk // 4):
            for col in range(residues // 256):
                yield functools.partial(products, k, quad, col)
        for begin in range(0, owned, 4):
            yield functools.partial(project, k, begin, 4)

    @pl.when(seq == sequences - 1)
    def _():
        pending = []
        last = max(STARTS) + far
        for tick in range(last + 1):
            for k in range(CHUNKS):
                t = tick - STARTS[k]
                if 0 <= t <= far:
                    step(1, k, t)
                    if t == far:
                        pending.extend(pieces(k))
                if tick == 0:
                    step(0, k, far)
            if tick == 0:
                send_left(1)
            if tick == 1:
                turn_weight()
            if tick == far - 2:
                arrange_left()
            for _ in range(5):
                if pending:
                    pending.pop(0)()
        for piece in pending:
            piece()
        sent = left_held.at[pl.ds(0, GROUPS * (devices - 1))]
        remote(sent, sent, left_send_sem, left_recv_sem.at[0], mate).wait_send()
        everything = held_ref.at[pl.ds(0, GROUPS * CHUNKS * (devices - 1))]
        remote(everything, everything, send_sem, mate_sem.at[0], mate).wait_send()


def block(
    devices,
    tokens,
    positions,
    target,
    emb,
    gain_one,
    wq,
    wk,
    wv,
    wg,
    gb,
    wo,
    table,
    gain_two,
    wl,
    wr,
    pair_weight,
    pair_bias,
):
    sequences, residues = tokens.shape
    features = target.shape[1]
    heads = table.shape[1]
    width = wl.shape[1]
    channels = pair_weight.shape[1]
    owned = residues // devices
    rings = devices // 2
    total = devices * sequences
    share = sequences // GROUPS
    operands = (
        tokens,
        positions[None, :],
        target,
        emb,
        gain_one[None, :],
        wq,
        wk,
        wv,
        wg,
        gb[None, :],
        wo,
        table.T,
        gain_two[None, :],
        wl.T,
        wr.T,
        pair_weight,
        pair_bias[None, :],
    )

    def const(a):
        return pl.BlockSpec(
            a.shape, lambda s: (0,) * a.ndim, pipeline_mode=pl.Buffered(buffer_count=1)
        )

    return pl.pallas_call(
        functools.partial(block_kernel, devices, heads),
        grid=(sequences,),
        in_specs=[const(a) for a in operands],
        out_specs=(
            pl.BlockSpec((1, residues, features), lambda s: (s, 0, 0)),
            pl.BlockSpec(memory_space=pltpu.VMEM),
        ),
        out_shape=(
            jax.ShapeDtypeStruct((sequences, residues, features), F32),
            jax.ShapeDtypeStruct((owned, residues, channels), F32),
        ),
        scratch_shapes=[
            pltpu.VMEM((heads, residues, residues), F32),
            pltpu.VMEM((heads, LANES), F32),
            pltpu.VMEM((share, LANES, features), BF16),
            pltpu.VMEM((4, features // LANES, width, LANES), F32),
            pltpu.VMEM((width * width, channels), F32),
            pltpu.VMEM((channels, width * width), BF16),
            pltpu.VMEM((LANES, features), BF16),
            pltpu.VMEM((4, residues, residues), F32),
            pltpu.VMEM((4, residues, residues), BF16),
            pltpu.VMEM((residues, features), F32),
            pltpu.VMEM((GROUPS * residues, LANES), F32),
            pltpu.VMEM((residues // LANES, width * sequences, LANES), F32),
            pltpu.VMEM((GROUPS * devices, owned, LANES), BF16),
            pltpu.VMEM((GROUPS * devices, owned, LANES), BF16),
            pltpu.VMEM((GROUPS * devices * owned, LANES), F32),
            pltpu.VMEM((4, owned * width, total), BF16),
            pltpu.VMEM((GROUPS * CHUNKS * devices, width * share // CHUNKS, residues), BF16),
            pltpu.VMEM((owned, (width // CHUNKS) * width, residues), BF16),
            pltpu.VMEM((owned, channels, residues), F32),
            pltpu.SemaphoreType.DMA,
            pltpu.SemaphoreType.DMA((GROUPS * CHUNKS, rings // 2)),
            pltpu.SemaphoreType.DMA((GROUPS * CHUNKS, rings // 2)),
            pltpu.SemaphoreType.DMA((GROUPS * CHUNKS,)),
            pltpu.SemaphoreType.DMA,
            pltpu.SemaphoreType.DMA((GROUPS,)),
        ],
        compiler_params=pltpu.CompilerParams(
            dimension_semantics=("arbitrary",),
            collective_id=0,
            has_side_effects=True,
            vmem_limit_bytes=60 << 20,
        ),
        cost_estimate=pl.CostEstimate(
            flops=27_000_000_000, bytes_accessed=14 << 20, transcendentals=17_000_000
        ),
        name="msa_block",
    )(*operands)


def shards(
    alignment_token_ids,
    residue_index_offsets,
    target_residue_feature,
    token_embedding_table,
    attention_norm_gain,
    query_weight,
    key_weight,
    value_weight,
    gate_weight,
    gate_offset_bias,
    output_weight,
    relative_position_table,
    product_norm_gain,
    left_weight,
    right_weight,
    pair_weight,
    pair_projection_bias,
):
    return block(
        lax.axis_size("wide"),
        alignment_token_ids,
        residue_index_offsets,
        target_residue_feature,
        token_embedding_table,
        attention_norm_gain,
        query_weight,
        key_weight,
        value_weight,
        gate_weight,
        gate_offset_bias,
        output_weight,
        relative_position_table,
        product_norm_gain,
        left_weight,
        right_weight,
        pair_weight,
        pair_projection_bias,
    )


def solution(mesh):
    placed = (
        P(("groups", "wide"), None),
        P("groups"),
        P("groups", None),
    ) + (P(),) * 14
    return jax.shard_map(
        shards,
        mesh=mesh,
        in_specs=placed,
        out_specs=(P(("groups", "wide"), None, None), P(("groups", "wide"), None, None)),
        check_vma=False,
    )
```
